256 devices in a mesh: group: 2 (over z), dp: 16 (over y, core), tensor: 8 (over x).
Axes of the slice: x: 8, y: 8, z: 2, core: 2. Of those that a mesh axis runs over, the one named last changes fastest.
The devices are a block of a 8x8x16 slice.
Arguments:
- tokens: bfloat16 [4096, 5120], P(('group', 'dp'), 'tensor'), parts along dimension 0, may hold values from -6 to 6
- router: bfloat16 [5120, 8], replicated, may hold values from -0.078125 to 0.078125
- expert_gate: bfloat16 [5120, 32768], P(None, ('dp', 'tensor')), may hold values from -0.078125 to 0.078125
- expert_up: bfloat16 [5120, 32768], P(None, ('dp', 'tensor')), may hold values from -0.078125 to 0.078125
- expert_down: bfloat16 [32768, 5120], P(('dp', 'tensor')), may hold values from -0.09375 to 0.09375
- shared_gate: bfloat16 [5120, 4096], P('dp', 'tensor'), may hold values from -0.078125 to 0.078125
- shared_up: bfloat16 [5120, 4096], P('dp', 'tensor'), may hold values from -0.078125 to 0.078125
- shared_down: bfloat16 [4096, 5120], P('tensor', 'dp'), may hold values from -0.09375 to 0.09375
- expert_ids: int32 [4096], P(('group', 'dp')), parts along dimension 0, may hold values from 0 to 7, as said below
- expert_slots: int32 [4096], P(('group', 'dp')), parts along dimension 0, may hold values from 0 to 31, as said below
Outputs:
- mixed: bfloat16 [4096, 5120], P(('group', 'dp'), 'tensor'), parts along dimension 0
The draws below stay inside these ranges and needn't reach their ends.
There are 2 independent parts, one for each index of `group`. The reference program is written for one: setup_inputs(seed, part) draws one part's arguments, and reference() takes and returns one part's arrays. A program takes and returns all parts, laid end to end along the dimension named above; an argument that names none is the same for every part. Nothing has to cross between parts.
Inputs may be any that keep to these rules, and one draw needn't show every extreme that they name: `expert_ids`: among the tokens of one index of dp no expert has more than 32; in every draw one expert has exactly 32 tokens from every index of dp. `expert_slots`: tokens of one index of dp with the same expert have distinct slots.
All inputs are finite; a program needn't handle non-finite values.
Results may differ from the reference program's by a relative error of at most 0.015.
Values may be sent and summed in bfloat16 or wider, within the bound.
A program may use at most 128 MiB of HBM per device.

```python
import jax
import jax.numpy as jnp
from jax import lax

D = 5120
FFE = 4096
FFS = 4096
TOK_DEV = 128
EXPERTS = 8
CAP = 32
TOKENS = 2048
N_DP = 16
N_TENSOR = 8


def routing_pairs(key):
    base = jax.random.fold_in(key, 101)
    busiest = jax.random.randint(jax.random.fold_in(base, 1), (), 0, EXPERTS)
    block_count = TOKENS // TOK_DEV
    pair_count = EXPERTS * CAP

    def one_block(block_key):
        rank_key, jitter_key, placing_key = jax.random.split(block_key, 3)
        pair_index = jnp.arange(pair_count, dtype=jnp.int32)
        expert = pair_index // CAP
        ranking = jax.random.permutation(rank_key, EXPERTS).astype(jnp.int32)
        jitter = jax.random.randint(jitter_key, (pair_count,), 0, 4096)
        scores = jitter + ranking[expert] * 512 + jnp.where(expert == busiest, 65536, 0)
        scores = scores * pair_count + pair_index
        chosen = lax.top_k(scores, TOK_DEV)[1].astype(jnp.int32)
        placing = jax.random.permutation(placing_key, TOK_DEV)
        expert_of = jnp.zeros((TOK_DEV,), jnp.int32).at[placing].set(chosen // CAP)
        slot_of = jnp.zeros((TOK_DEV,), jnp.int32).at[placing].set(chosen % CAP)
        return (expert_of, slot_of)
    block_keys = jax.random.split(jax.random.fold_in(base, 2), block_count)
    expert_of, slot_of = jax.vmap(one_block)(block_keys)
    return (expert_of.reshape(TOKENS), slot_of.reshape(TOKENS))


def draw_expert_ids(key, part):
    return routing_pairs(key)[0]


def draw_expert_slots(key, part):
    return routing_pairs(key)[1]


def levels(rng, extent, shards, low, high):
    def one(axis_at, parts):
        draws = jax.random.uniform(jax.random.fold_in(jax.random.fold_in(rng, 6), axis_at), (parts,), jnp.float32, low / len(shards), high / len(shards))
        return jnp.repeat(jnp.exp(draws), extent[axis_at] // parts).reshape((-1,) + (1,) * (len(extent) - axis_at - 1))

    factor_of = one(*shards[0])
    for cut in shards[1:]:
        factor_of = factor_of * one(*cut)
    return factor_of


def gaussian(rng, dims, deviation, limit, cuts=(), held_as=jnp.bfloat16):
    result = jax.random.normal(rng, dims, jnp.float32) * deviation
    if len(cuts) > 0:
        result = levels(rng, dims, cuts, -0.22, 0.18) * result
    return jnp.clip(result, min=-limit, max=limit).astype(held_as)


def setup_inputs(seed: int = 0, part: int = 0) -> dict:
    splits = jax.random.split(jax.random.key(seed), 11)
    part_splits = jax.random.split(jax.random.fold_in(splits[10], part), 11)
    return {
        "tokens": gaussian(part_splits[0], (TOKENS, D), 1.0, 6.0, ((0, 16), (1, 8))),
        "router": gaussian(splits[1], (D, EXPERTS), D ** -0.5, 0.078125),
        "expert_gate": gaussian(splits[2], (D, EXPERTS * FFE), D ** -0.5, 0.078125, ((1, 128),)),
        "expert_up": gaussian(splits[3], (D, EXPERTS * FFE), D ** -0.5, 0.078125, ((1, 128),)),
        "expert_down": gaussian(splits[4], (EXPERTS * FFE, D), FFE ** -0.5, 0.09375, ((0, 128),)),
        "shared_gate": gaussian(splits[5], (D, FFS), D ** -0.5, 0.078125, ((0, 16), (1, 8))),
        "shared_up": gaussian(splits[6], (D, FFS), D ** -0.5, 0.078125, ((0, 16), (1, 8))),
        "shared_down": gaussian(splits[7], (FFS, D), FFS ** -0.5, 0.09375, ((0, 8), (1, 16))),
        "expert_ids": draw_expert_ids(jax.random.fold_in(jax.random.fold_in(splits[10], part), 71), part),
        "expert_slots": draw_expert_slots(jax.random.fold_in(jax.random.fold_in(splits[10], part), 71), part),
    }


def rounded_blocks(hidden, weight, block_count):
    row_count = hidden.shape[0]
    block_width = hidden.shape[1] // block_count
    hidden_blocks = hidden.reshape(row_count, block_count, block_width).transpose(1, 0, 2)
    weight_blocks = weight.reshape(block_count, block_width, weight.shape[1])

    def accumulate(running, inputs):
        portion = jnp.dot(inputs[0], inputs[1], preferred_element_type=jnp.float32).astype(jnp.bfloat16)
        portion = lax.optimization_barrier(portion)
        return running + portion.astype(jnp.float32), None

    running, _ = lax.scan(accumulate, jnp.zeros((row_count, weight.shape[1]), jnp.float32), (hidden_blocks, weight_blocks))
    return running


def reference(tokens, router, expert_gate, expert_up, expert_down, shared_gate, shared_up, shared_down, expert_ids, expert_slots):
    logits = jnp.dot(tokens, router, preferred_element_type=jnp.float32)
    one_hot = (expert_ids[:, None] == jnp.arange(EXPERTS, dtype=jnp.int32)[None, :]).astype(jnp.float32)
    gating = jax.nn.sigmoid(jnp.sum(logits * one_hot, axis=1))
    routed = (tokens.astype(jnp.float32) * gating[:, None]).astype(jnp.bfloat16)
    source_index = (jnp.arange(TOKENS, dtype=jnp.int32) // TOK_DEV).astype(jnp.int32)
    slot_row = (source_index * CAP + expert_slots).astype(jnp.int32)
    slot_table = jnp.zeros((EXPERTS, N_DP * CAP, D), jnp.bfloat16).at[expert_ids, slot_row].set(routed)
    gate_stack = expert_gate.reshape(D, EXPERTS, FFE).transpose(1, 0, 2)
    up_stack = expert_up.reshape(D, EXPERTS, FFE).transpose(1, 0, 2)
    down_stack = expert_down.reshape(EXPERTS, FFE, D)

    def one_expert(inputs):
        table, gate_w, up_w, down_w = inputs
        gate_sum = jnp.dot(table, gate_w, preferred_element_type=jnp.float32)
        up_sum = jnp.dot(table, up_w, preferred_element_type=jnp.float32)
        expert_hidden = (jax.nn.silu(gate_sum) * up_sum).astype(jnp.bfloat16)
        return rounded_blocks(expert_hidden, down_w, 2 * N_TENSOR).astype(jnp.bfloat16)

    expert_table = lax.map(one_expert, (slot_table, gate_stack, up_stack, down_stack))
    expert_out = expert_table[expert_ids, slot_row]
    shared_gate_sum = jnp.dot(tokens, shared_gate, preferred_element_type=jnp.float32)
    shared_up_sum = jnp.dot(tokens, shared_up, preferred_element_type=jnp.float32)
    shared_hidden = (jax.nn.silu(shared_gate_sum) * shared_up_sum).astype(jnp.bfloat16)
    shared_out = rounded_blocks(shared_hidden, shared_down, N_TENSOR)
    return (shared_out + expert_out.astype(jnp.float32)).astype(jnp.bfloat16)
```

```python
import functools

import jax
import jax.numpy as jnp
from jax import lax
from jax.experimental import pallas as pl
from jax.experimental.pallas import tpu as pltpu
from jax.sharding import PartitionSpec as P

MESH = pl.DeviceIdType.MESH
BF16 = jnp.bfloat16
F32 = jnp.float32


def dot(a, b):
    return jnp.dot(a, b, preferred_element_type=F32)


def dot_turned(a, b):
    return lax.dot_general(a, b, (((1,), (1,)), ((), ())), preferred_element_type=F32)


class Sems:
    def __init__(self, send, recv, local):
        self.send, self.recv, self.local = send, recv, local
        self.used, self.local_used, self.started = 0, 0, []

    def number(self):
        self.used += 1
        return self.used - 1

    def copy(self, number, src, dst, device):
        return pltpu.make_async_remote_copy(
            src_ref=src,
            dst_ref=dst,
            send_sem=self.send.at[number],
            recv_sem=self.recv.at[number],
            device_id=device,
            device_id_type=MESH,
        )

    def start(self, number, src, dst, device):
        copy = self.copy(number, src, dst, device)
        copy.start()
        self.started.append(copy)

    def arrived(self, number, dst, device):
        self.copy(number, dst, dst, device).wait_recv()

    def load(self, src, dst):
        copy = pltpu.make_async_copy(src, dst, self.local.at[self.local_used])
        self.local_used += 1
        copy.start()
        return copy


class Gather:
    def __init__(self, sems, n, me, device_of, region, partner=None):
        self.sems, self.n, self.me, self.half = sems, n, me, n // 2
        self.device_of, self.region, self.partner = device_of, region, partner
        self.numbers = {(k, way, part): sems.number() for k, way, part in self.steps()}
        if partner is not None:
            self.relays = {step: sems.number() for step in [(0, 1, 0), (0, 1, 1), *self.steps()]}

    def carries(self, k, way, part):
        return k < self.half or (k == self.half and part == (0 if way == 1 else 1))

    def steps(self):
        return [
            (k, way, part)
            for k in range(1, self.half + 1)
            for part in (0, 1)
            for way in (1, -1)
            if self.carries(k, way, part)
        ]

    def at(self, offset):
        return lax.rem(self.me + offset + self.n, self.n)

    def send(self, k, way, part):
        if self.carries(k, way, part):
            ref = self.region(self.at(-way * (k - 1)), part, False)
            self.sems.start(self.numbers[k, way, part], ref, ref, self.device_of(self.at(way)))

    def relay(self, k, way, part):
        ref = self.region(self.at(-way * k), part, False)
        self.sems.start(self.relays[k, way, part], ref, ref, self.partner)

    def take(self, k, way, part):
        if self.carries(k, way, part):
            ref = self.region(self.at(-way * k), part, False)
            self.sems.arrived(self.numbers[k, way, part], ref, self.device_of(self.at(-way)))
            if self.partner is not None:
                self.relay(k, way, part)

    def take_on(self, k, part):
        for way in (1, -1):
            if self.carries(k, way, part):
                self.take(k, way, part)
                self.send(k + 1, way, part)

    def relayed(self, k, way):
        for part in (0, 1):
            if k == 0 or self.carries(k, way, part):
                ref = self.region(self.at(-way * k), part, True)
                self.sems.arrived(self.relays[k, way, part], ref, self.partner)


def kernel(
    sizes,
    ids_ref,
    slots_ref,
    tok_hbm,
    router_hbm,
    eg_hbm,
    eu_hbm,
    ed_hbm,
    sg_hbm,
    su_hbm,
    sd_hbm,
    out_ref,
    tok,
    router,
    eg,
    eu,
    ed,
    sg,
    su,
    sd,
    outgoing,
    slot,
    gate_acc,
    up_acc,
    logit_acc,
    hidden,
    own_sum,
    pair_send,
    pair_recv,
    ring_send,
    ring_recv,
    back_send,
    back_recv,
    sgate_acc,
    sup_acc,
    shidden,
    shared_recv,
    shared_send,
    send_sems,
    recv_sems,
    local_sems,
):
    nx, ny, cap = sizes
    half = nx // 2
    toks, width = out_ref.shape
    rows = ny * cap
    part_rows = rows // 2
    krows = sg_hbm.shape[0]
    x = lax.axis_index("tensor")
    d = lax.axis_index("dp")
    core = lax.rem(d, 2)
    y = lax.div(d, 2)
    other = 1 - core
    partner = {"dp": 2 * y + other}
    along_x = lambda i: {"tensor": i}
    along_y = lambda i: {"dp": 2 * i + core}
    at_x = lambda o: lax.rem(x + o + nx, nx)
    at_y = lambda o: lax.rem(y + o + ny, ny)
    sems = Sems(send_sems, recv_sems, local_sems)

    load_tok = sems.load(tok_hbm, tok.at[x])
    my_k = pl.ds(pl.multiple_of(core * krows, krows), krows)
    load_g = sems.load(sg_hbm, sg.at[y, my_k])
    load_u = sems.load(su_hbm, su.at[y, my_k])
    load_d = sems.load(sd_hbm, sd.at[y, my_k])
    load_e = [sems.load(router_hbm, router), sems.load(eg_hbm, eg), sems.load(eu_hbm, eu)]
    load_ed = [sems.load(ed_hbm.at[:, i * width : (i + 1) * width], ed.at[i]) for i in range(nx)]

    barrier = pltpu.get_barrier_semaphore()
    peers = [along_x(at_x(o)) for o in range(1, nx)] + [along_y(at_y(o)) for o in range(1, ny)] + [partner]
    for peer in peers:
        pl.semaphore_signal(barrier, inc=1, device_id=peer, device_id_type=MESH)

    index = ids_ref[...] * cap + slots_ref[...]
    pick = (lax.broadcasted_iota(jnp.int32, (rows, toks), 0) == index).astype(F32).astype(BF16)
    load_tok.wait()
    outgoing[...] = dot(pick, tok[x]).astype(BF16).reshape(ny, cap, width)

    def source_rows(source, of_core):
        return pl.ds(pl.multiple_of(of_core * rows + source * cap, cap), cap)

    slot[x, source_rows(y, core), :] = outgoing[y]

    def core_half(extent, part, swap):
        base = (other if swap else core) * extent + part * (extent // 2)
        return pl.ds(pl.multiple_of(base, extent // 2), extent // 2)

    tok_ring = Gather(
        sems, nx, x, along_x, lambda i, part, swap: tok.at[i, pl.ds(part * (toks // 2), toks // 2)]
    )
    slot_ring = Gather(
        sems, nx, x, along_x, lambda i, part, swap: slot.at[i, core_half(rows, part, swap)], partner
    )

    def wide(i, part, swap):
        base = (other if swap else core) * krows
        return (su if part else sg).at[i, pl.ds(pl.multiple_of(base, krows), krows)]

    wide_ring = Gather(sems, ny, y, along_y, wide, partner)
    def tall(i, part, swap):
        base = (other if swap else core) * krows + part * (krows // 2)
        return sd.at[i, pl.ds(pl.multiple_of(base, krows // 2), krows // 2)]

    down_ring = Gather(sems, ny, y, along_y, tall, partner)
    both = (1, -1)

    far_first = sorted(range(1, ny), key=lambda o: -min(o, ny - o))
    dispatch = {o: sems.number() for o in range(1, ny)}
    back = {o: sems.number() for o in range(1, ny)}
    pl.semaphore_wait(barrier, len(peers))

    for o in far_first:
        sems.start(
            dispatch[o], outgoing.at[at_y(o)], slot.at[x, source_rows(y, core)], along_y(at_y(o))
        )
    for part in (0, 1):
        for way in both:
            tok_ring.send(1, way, part)
    for part, load in ((0, load_g), (1, load_u)):
        load.wait()
        for way in both:
            wide_ring.send(1, way, part)
        wide_ring.relay(0, 1, part)

    for part in (0, 1):
        tok_ring.take_on(1, part)
    load_d.wait()
    for part in (0, 1):
        for way in both:
            down_ring.send(1, way, part)
        down_ring.relay(0, 1, part)
    for k in range(2, half):
        for part in (0, 1):
            tok_ring.take_on(k, part)

    for o in range(1, ny):
        sems.arrived(dispatch[o], slot.at[x, source_rows(at_y(-o), core)], along_y(at_y(-o)))
    for part in (0, 1):
        for way in both:
            slot_ring.send(1, way, part)
        slot_ring.relay(0, 1, part)
    for part in (0, 1):
        tok_ring.take_on(half, part)

    for load in load_e:
        load.wait()

    def expert_chunk(i, first=False):
        at = pl.ds(pl.multiple_of(i * width, width), width)
        terms = (dot(slot[i], eg[at, :]), dot(slot[i], eu[at, :]), dot_turned(slot[i], router[:, at]))
        for acc, term in zip((gate_acc, up_acc, logit_acc), terms):
            acc[...] = term if first else acc[...] + term

    def shared_chunk(i, first=False):
        for acc, weight in ((sgate_acc, sg), (sup_acc, su)):
            term = dot(tok[i], weight[i])
            acc[...] = term if first else acc[...] + term

    slot_ring.relayed(0, 1)
    expert_chunk(x, True)
    wide_ring.relayed(0, 1)
    shared_chunk(y, True)

    def take_slots(k):
        for part in (0, 1):
            slot_ring.take_on(k, part)

    def multiply_slots(k):
        for way in both:
            slot_ring.relayed(k, way)
        for way in both if k < half else (1,):
            expert_chunk(at_x(-way * k))

    def multiply_wide(k):
        for way in both:
            wide_ring.relayed(k, way)
        for way in both if k < half else (1,):
            shared_chunk(at_y(-way * k))

    wide_ring.take_on(1, 0)
    take_slots(1)
    wide_ring.take_on(1, 1)
    multiply_slots(1)
    if half > 2:
        take_slots(2)
        wide_ring.take_on(2, 0)
        multiply_wide(1)
        multiply_slots(2)
    for k in range(3, half):
        take_slots(k)
        wide_ring.take_on(k - 1, 1)
        multiply_slots(k)
    take_slots(half)
    multiply_slots(half)

    lane = lax.broadcasted_iota(jnp.int32, logit_acc.shape, 1)
    logit = jnp.sum(jnp.where(lane == y, logit_acc[...], 0.0), axis=1, keepdims=True)
    factor = jax.nn.sigmoid(logit)
    gate_value = gate_acc[...] * factor
    hidden[...] = (jax.nn.silu(gate_value) * (up_acc[...] * factor)).astype(BF16)
    for load in load_ed:
        load.wait()

    offsets = [half] + [way * k for k in range(half - 1, 0, -1) for way in both] + [0]
    pairs = [sems.number() for _ in offsets]
    hops = {
        (k, way, part): sems.number()
        for k in range(1, half + 1)
        for way in both
        for part in (0, 1)
        if k < half or part == (0 if way == 1 else 1)
    }
    keep_slots = pl.ds(pl.multiple_of(core * rows, rows), rows)
    give_slots = pl.ds(pl.multiple_of(other * rows, rows), rows)
    direction = {1: 0, -1: 1}

    def down_block(at):
        block = ed[at_x(offsets[at])]
        pair_send[at] = dot(hidden[give_slots, :], block).astype(BF16)
        sems.start(pairs[at], pair_send.at[at], pair_recv.at[at], partner)
        own_sum[at] = dot(hidden[keep_slots, :], block)

    def arrived_hop(k, way, part):
        ref = ring_recv.at[direction[way], k - 1, pl.ds(part * part_rows, part_rows)]
        sems.arrived(hops[k, way, part], ref, along_x(at_x(-way)))
        return ref[...].astype(F32)

    def pass_on(at, part):
        offset = offsets[at]
        k = abs(offset)
        part_at = pl.ds(part * part_rows, part_rows)
        value = own_sum[at, part_at, :] + pair_recv[at, part_at, :].astype(F32)
        if offset == 0:
            for way in both:
                value += arrived_hop(1, way, part)
            back_send[part_at, :] = value.astype(BF16)
            return
        way = (1 if part == 0 else -1) if k == half else (1 if offset > 0 else -1)
        if k < half and (k + 1, way, part) in hops:
            value += arrived_hop(k + 1, way, part)
        place = (direction[way], k - 1, part_at)
        ring_send[place] = value.astype(BF16)
        sems.start(hops[k, way, part], ring_send.at[place], ring_recv.at[place], along_x(at_x(way)))

    def paired(at):
        sems.arrived(pairs[at], pair_recv.at[at], partner)

    down_block(0)
    down_block(1)
    paired(0)
    for part in (0, 1):
        pass_on(0, part)
    down_block(2)
    for k in range(2, half):
        wide_ring.take_on(k, 0) if k > 2 or half == 2 else None
    for at in range(3, len(offsets)):
        down_block(at)
    for at in range(1, len(offsets)):
        paired(at)
    for part in (0, 1):
        pass_on(1, part)
        pass_on(2, 1 - part)
    if half > 2:
        wide_ring.take_on(half - 1, 1)
        multiply_wide(half - 2)
    if half > 2:
        for part in (0, 1):
            pass_on(3, part)
            pass_on(4, part)
        multiply_wide(half - 1)
    else:
        multiply_wide(1)
    for way in both:
        for part in (0, 1):
            down_ring.take(1, way, part)
            down_ring.send(2, way, part)
    for part in (0, 1):
        wide_ring.take_on(half, part)
    for k in range(half - 3, 0, -1):
        at = 1 + 2 * (half - 1 - k)
        for part in (0, 1):
            pass_on(at, part)
            pass_on(at + 1, part)
    multiply_wide(half)
    shidden[...] = (jax.nn.silu(sgate_acc[...]) * sup_acc[...]).astype(BF16)

    out_sent = [sems.number() for _ in range(ny)]
    out_came = [sems.number() for _ in range(nx)]
    shared_copies = []

    def shared_block(offset):
        place = at_y(offset)
        value = dot_turned(shidden[...], sd[place]).astype(BF16)
        shared_send[place] = value
        copy = pltpu.make_async_remote_copy(
            src_ref=shared_send.at[place],
            dst_ref=shared_recv.at[x],
            send_sem=send_sems.at[out_sent[offset + ny // 2]],
            recv_sem=recv_sems.at[out_came[0] + x],
            device_id=along_x(place),
            device_id_type=MESH,
        )
        pl.when(place != x)(copy.start)
        shared_copies.append((place, copy))

    def down_blocks(k):
        for way in both if 0 < k < ny // 2 else (1,):
            if k:
                down_ring.relayed(k, way)
                if k == ny // 2:
                    down_ring.relayed(k, -1)
            else:
                down_ring.relayed(0, 1)
            shared_block(-way * k)

    down_blocks(0)
    down_blocks(1)
    for k in range(2, half):
        for part in (0, 1):
            down_ring.take_on(k, part)
        down_blocks(k)
    for part in (0, 1):
        pass_on(len(offsets) - 1, part)
    for o in far_first:
        sems.start(
            back[o], back_send.at[pl.ds(pl.multiple_of(at_y(o) * cap, cap), cap)], back_recv.at[y], along_y(at_y(o))
        )
    back_recv[y] = back_send[pl.ds(pl.multiple_of(y * cap, cap), cap), :]
    for part in (0, 1):
        down_ring.take_on(half, part)
    down_blocks(half)
    total = shared_send[x].astype(F32)

    for o in range(1, ny):
        sems.arrived(back[o], back_recv.at[at_y(-o)], along_y(at_y(-o)))
    total += lax.dot_general(
        pick, back_recv[...].reshape(rows, width), (((0,), (0,)), ((), ())), preferred_element_type=F32
    )
    for o in range(1, nx):
        i = at_x(-o)
        sems.arrived(out_came[0] + i, shared_recv.at[i], along_x(i))
        total += shared_recv[i].astype(F32)
    out_ref[...] = total.astype(BF16)
    for copy in sems.started:
        copy.wait_send()
    for place, copy in shared_copies:
        pl.when(place != x)(copy.wait_send)


def on_device(nx, ndp, tokens, router, eg, eu, ed, sg, su, sd, ids, slots):
    toks, width = tokens.shape
    ny = ndp // 2
    cap = min(2 * toks // ny, toks // 2)
    rows = ny * cap
    units = eg.shape[1]
    hid = sg.shape[1]
    features = eg.shape[0]
    krows = sg.shape[0]
    half = nx // 2
    vmem = lambda *shape, dtype=BF16: pltpu.VMEM(shape, dtype)
    any_space = pl.BlockSpec(memory_space=pl.ANY)
    in_vmem = pl.BlockSpec(memory_space=pltpu.VMEM)
    return pl.pallas_call(
        functools.partial(kernel, (nx, ny, cap)),
        out_shape=jax.ShapeDtypeStruct((toks, width), BF16),
        in_specs=[in_vmem] * 2 + [any_space] * 8,
        out_specs=in_vmem,
        scratch_shapes=[
            vmem(nx, toks, width),
            vmem(router.shape[1], features),
            vmem(features, units),
            vmem(features, units),
            vmem(nx, units, width),
            vmem(ny, 2 * krows, hid),
            vmem(ny, 2 * krows, hid),
            vmem(ny, 2 * krows, hid),
            vmem(ny, cap, width),
            vmem(nx, 2 * rows, width),
            vmem(2 * rows, units, dtype=F32),
            vmem(2 * rows, units, dtype=F32),
            vmem(2 * rows, router.shape[1], dtype=F32),
            vmem(2 * rows, units),
            vmem(nx, rows, width, dtype=F32),
            vmem(nx, rows, width),
            vmem(nx, rows, width),
            vmem(2, half, rows, width),
            vmem(2, half, rows, width),
            vmem(rows, width),
            vmem(ny, cap, width),
            vmem(toks, hid, dtype=F32),
            vmem(toks, hid, dtype=F32),
            vmem(toks, hid),
            vmem(nx, toks, width),
            vmem(nx, toks, width),
            pltpu.SemaphoreType.DMA((192,)),
            pltpu.SemaphoreType.DMA((192,)),
            pltpu.SemaphoreType.DMA((32,)),
        ],
        compiler_params=pltpu.CompilerParams(
            collective_id=0, has_side_effects=True, vmem_limit_bytes=66_000_000
        ),
        name="layer",
    )(ids.reshape(1, toks), slots.reshape(1, toks), tokens, router.T, eg, eu, ed, sg, su, sd.T)


def solution(mesh):
    in_specs = (
        P(("group", "dp"), "tensor"),
        P(),
        P(None, ("dp", "tensor")),
        P(None, ("dp", "tensor")),
        P(("dp", "tensor"), None),
        P("dp", "tensor"),
        P("dp", "tensor"),
        P("tensor", "dp"),
        P(("group", "dp")),
        P(("group", "dp")),
    )
    return jax.shard_map(
        functools.partial(on_device, mesh.shape["tensor"], mesh.shape["dp"]),
        mesh=mesh,
        in_specs=in_specs,
        out_specs=P(("group", "dp"), "tensor"),
        check_vma=False,
    )
```
